32 devices in a mesh: tp: 4 (over z), dp: 8 (over y, x, core).
Axes of the slice: x: 2, y: 2, z: 4, core: 2. Of those that a mesh axis runs over, the one named last changes fastest.
Arguments:
- x_saved: bfloat16 [8, 768, 4096], P('dp', 'tp')
- dy_out: bfloat16 [8, 768, 4096], P('dp', 'tp')
- ln_params: float32 [4, 4096], replicated
- w_qkv: bfloat16 [4096, 8, 6, 128], P(None, 'tp')
- w_out: bfloat16 [4096, 4096], P('tp')
- w_up: bfloat16 [4096, 16384], P(None, 'tp')
- w_down: bfloat16 [16384, 4096], P('tp')
Outputs:
- output 1: bfloat16 [8, 768, 4096], P('dp', 'tp')
- output 2: float32 [4, 4096], replicated
- output 3: float32 [4096, 8, 6, 128], P('dp', 'tp')
- output 4: float32 [4096, 4096], P(('tp', 'dp'))
- output 5: float32 [4096, 16384], P('dp', 'tp')
- output 6: float32 [16384, 4096], P(('tp', 'dp'))
All inputs are finite; a program needn't handle non-finite values.
Results may differ from the reference program's by a relative error of at most 0.0111644.
Values are sent between devices in bfloat16 or wider.
A program may use at most 1 GiB of HBM per device.

```python
import jax
import jax.numpy as jnp
from jax import lax

NUM_SEQS = 8
SEQ_LEN = 768
D_MODEL = 4096
NUM_HEADS = 32
KV_HEADS = 8
HEAD_DIM = 128
FF_DIM = 16384
Q_PER_GROUP = NUM_HEADS // KV_HEADS
NORM_EPS = 1e-5
ROPE_BASE = 10000.0


def layer_norm(x_rows, norm_gain, norm_shift):
    row_mean = jnp.mean(x_rows, axis=-1, keepdims=True)
    centered = x_rows - row_mean
    row_var = jnp.mean(centered * centered, axis=-1, keepdims=True)
    return (centered * lax.rsqrt(row_var + NORM_EPS) * norm_gain + norm_shift).astype(jnp.bfloat16)


def rope_tables(positions):
    half_dim = HEAD_DIM // 2
    inv_freq = ROPE_BASE ** (-2.0 * jnp.arange(half_dim, dtype=jnp.float32) / HEAD_DIM)
    angles = positions.astype(jnp.float32)[:, None] * inv_freq[None, :]
    return jnp.cos(angles), jnp.sin(angles)


def apply_rope(tensor, cos_t, sin_t):
    half_dim = tensor.shape[-1] // 2
    t_f32 = tensor.astype(jnp.float32)
    lo_half = t_f32[..., :half_dim]
    hi_half = t_f32[..., half_dim:]
    return jnp.concatenate([lo_half * cos_t - hi_half * sin_t, hi_half * cos_t + lo_half * sin_t], axis=-1).astype(jnp.bfloat16)


def attention(qkv_proj):
    positions = jnp.arange(SEQ_LEN)
    cos_t, sin_t = rope_tables(positions)
    rotated = apply_rope(qkv_proj[:, :, :Q_PER_GROUP + 1, :], cos_t[:, None, None, :], sin_t[:, None, None, :])
    query_rot = rotated[:, :, :Q_PER_GROUP, :]
    key_rot = rotated[:, :, Q_PER_GROUP, :]
    values = qkv_proj[:, :, Q_PER_GROUP + 1, :]
    scores = jnp.einsum('tgqh,sgh->gqts', query_rot.astype(jnp.float32), key_rot.astype(jnp.float32)) * (HEAD_DIM ** -0.5)
    causal = positions[:, None] >= positions[None, :]
    attn_probs = jax.nn.softmax(jnp.where(causal, scores, -1e30), axis=-1).astype(jnp.bfloat16)
    return jnp.einsum('gqts,sgh->tgqh', attn_probs.astype(jnp.float32), values.astype(jnp.float32)).astype(jnp.bfloat16)


def layer_forward(x_seq, ln_params, w_qkv, w_out, w_up, w_down):
    x_f32 = x_seq.astype(jnp.float32)
    h_attn = layer_norm(x_f32, ln_params[0], ln_params[1])
    h_mlp = layer_norm(x_f32, ln_params[2], ln_params[3])
    qkv_proj = jnp.dot(h_attn.astype(jnp.float32), w_qkv.reshape(D_MODEL, -1), preferred_element_type=jnp.float32).astype(jnp.bfloat16)
    context = attention(qkv_proj.reshape(SEQ_LEN, KV_HEADS, Q_PER_GROUP + 2, HEAD_DIM))
    attn_out = jnp.dot(context.reshape(SEQ_LEN, NUM_HEADS * HEAD_DIM).astype(jnp.float32), w_out, preferred_element_type=jnp.float32)
    hidden = jnp.dot(h_mlp.astype(jnp.float32), w_up, preferred_element_type=jnp.float32).astype(jnp.bfloat16)
    gelu_out = jax.nn.gelu(hidden.astype(jnp.float32), approximate=False).astype(jnp.bfloat16)
    mlp_out = jnp.dot(gelu_out.astype(jnp.float32), w_down, preferred_element_type=jnp.float32)
    return x_f32 + attn_out + mlp_out


def setup_inputs(seed: int = 0) -> dict:
    key_list = jax.random.split(jax.random.key(seed), 8)
    act_shape = (NUM_SEQS, SEQ_LEN, D_MODEL)
    x_saved = jax.random.normal(key_list[0], act_shape, jnp.float32)
    shared_dir = jax.random.normal(key_list[1], (NUM_SEQS, 1, D_MODEL), jnp.float32)
    dy_out = 0.6 * shared_dir + 0.8 * jax.random.normal(key_list[2], act_shape, jnp.float32)
    ln_base = jnp.array([1.0, 0.0, 1.0, 0.0], jnp.float32)[:, None]
    ln_spread = jnp.array([0.3, 0.5, 0.3, 0.5], jnp.float32)[:, None]
    ln_params = ln_base + ln_spread * jax.random.normal(key_list[3], (4, D_MODEL), jnp.float32)
    w_qkv = jax.random.normal(key_list[4], (D_MODEL, KV_HEADS, Q_PER_GROUP + 2, HEAD_DIM), jnp.float32) * D_MODEL ** -0.5
    w_out = jax.random.normal(key_list[5], (NUM_HEADS * HEAD_DIM, D_MODEL), jnp.float32) * (NUM_HEADS * HEAD_DIM) ** -0.5
    w_up = jax.random.normal(key_list[6], (D_MODEL, FF_DIM), jnp.float32) * D_MODEL ** -0.5
    w_down = jax.random.normal(key_list[7], (FF_DIM, D_MODEL), jnp.float32) * FF_DIM ** -0.5
    return {'x_saved': x_saved.astype(jnp.bfloat16), 'dy_out': dy_out.astype(jnp.bfloat16), 'ln_params': ln_params, 'w_qkv': w_qkv.astype(jnp.bfloat16), 'w_out': w_out.astype(jnp.bfloat16), 'w_up': w_up.astype(jnp.bfloat16), 'w_down': w_down.astype(jnp.bfloat16)}


def reference(x_saved, dy_out, ln_params, w_qkv, w_out, w_up, w_down):
    weights = (ln_params, w_qkv.astype(jnp.float32), w_out.astype(jnp.float32), w_up.astype(jnp.float32), w_down.astype(jnp.float32))

    def seq_step(grad_sums, seq_pair):
        x_seq, dy_seq = seq_pair
        _, pull_back = jax.vjp(layer_forward, x_seq, *weights)
        grads = pull_back(dy_seq.astype(jnp.float32))
        return tuple(grad_total + grad_part for grad_total, grad_part in zip(grad_sums, grads[1:])), grads[0]

    zero_sums = tuple(jnp.zeros_like(weight) for weight in weights)
    grad_sums, grad_x = lax.scan(seq_step, zero_sums, (x_saved, dy_out))
    return (grad_x, grad_sums[0], grad_sums[1], grad_sums[2], grad_sums[3], grad_sums[4])
```

```python
import jax
import jax.numpy as jnp
from jax import lax
from jax.sharding import PartitionSpec as P

NORM_EPS = 1e-5
ROPE_BASE = 10000.0
CORE, XAX, YAX = 1, 2, 4
F32, BF16 = jnp.float32, jnp.bfloat16


def norm_stats(x_rows):
    row_mean = jnp.mean(x_rows, axis=-1, keepdims=True)
    centered = x_rows - row_mean
    row_var = jnp.mean(centered * centered, axis=-1, keepdims=True)
    return row_mean, lax.rsqrt(row_var + NORM_EPS)


def norm_apply(x_rows, row_mean, row_rstd, norm_gain, norm_shift):
    return ((x_rows.astype(F32) - row_mean) * row_rstd * norm_gain + norm_shift).astype(BF16)


def layer_norm(x_rows, norm_gain, norm_shift):
    row_mean, row_rstd = norm_stats(x_rows)
    return norm_apply(x_rows, row_mean, row_rstd, norm_gain, norm_shift)


def rope_tables(positions, head_dim):
    half_dim = head_dim // 2
    inv_freq = ROPE_BASE ** (-2.0 * jnp.arange(half_dim, dtype=F32) / head_dim)
    angles = positions.astype(F32)[:, None] * inv_freq[None, :]
    return jnp.cos(angles), jnp.sin(angles)


def apply_rope(tensor, cos_t, sin_t):
    half_dim = tensor.shape[-1] // 2
    t_f32 = tensor.astype(F32)
    lo_half = t_f32[..., :half_dim]
    hi_half = t_f32[..., half_dim:]
    return jnp.concatenate([lo_half * cos_t - hi_half * sin_t, hi_half * cos_t + lo_half * sin_t], axis=-1).astype(BF16)


def attention_core(qkv_proj, cos_t, sin_t):
    q_slots = qkv_proj.shape[3] - 2
    positions = jnp.arange(qkv_proj.shape[1])
    rotated = apply_rope(qkv_proj[:, :, :, :q_slots + 1, :], cos_t[:, None, None, :], sin_t[:, None, None, :])
    query_rot = rotated[:, :, :, :q_slots, :]
    key_rot = rotated[:, :, :, q_slots, :]
    values = qkv_proj[:, :, :, q_slots + 1, :]
    scores = jnp.einsum('btgqh,bsgh->bgqts', query_rot, key_rot, preferred_element_type=F32) * (qkv_proj.shape[4] ** -0.5)
    causal = positions[:, None] >= positions[None, :]
    attn_probs = jax.nn.softmax(jnp.where(causal, scores, -1e30), axis=-1).astype(BF16)
    return jnp.einsum('bgqts,bsgh->btgqh', attn_probs, values, preferred_element_type=F32).astype(BF16)


def swap(value, bit):
    return lax.ppermute(value, 'dp', [(i, i ^ bit) for i in range(8)])


def swap_tp(value, bit):
    return lax.ppermute(value, 'tp', [(i, i ^ bit) for i in range(4)])


def hold(*values):
    return lax.optimization_barrier(values)


def mm(spec, lhs, rhs):
    return jnp.einsum(spec, lhs, rhs, preferred_element_type=F32)


def solution(mesh):
    def local_body(x_in, dy_in, ln_params, w_qkv, w_out, w_up, w_down):
        x_loc, dy_loc = x_in[0], dy_in[0]
        me = lax.axis_index('dp')
        my_c, my_x, my_y = me % 2, (me // 2) % 2, me // 4

        def shares_x(arr, x_at, c_at):
            width = arr.shape[1] // 8
            pick = lambda y: lax.dynamic_slice_in_dim(arr, (y * 4 + x_at * 2 + c_at) * width, width, 1)
            return jnp.concatenate([pick(my_y), pick(1 - my_y)], axis=1)

        def shares_y(arr, y_at, c_at):
            width = arr.shape[1] // 8
            pick = lambda x: lax.dynamic_slice_in_dim(arr, (y_at * 4 + x * 2 + c_at) * width, width, 1)
            return jnp.concatenate([pick(my_x), pick(1 - my_x)], axis=1)

        def spread_x(arr):
            return [shares_x(arr, my_x, my_c), swap(shares_x(arr, my_x, 1 - my_c), CORE),
                    swap(shares_x(arr, 1 - my_x, my_c), XAX),
                    swap(shares_x(arr, 1 - my_x, 1 - my_c), XAX | CORE)]

        def spread_y(arr):
            return [shares_y(arr, my_y, my_c), swap(shares_y(arr, my_y, 1 - my_c), CORE),
                    swap(shares_y(arr, 1 - my_y, my_c), YAX),
                    swap(shares_y(arr, 1 - my_y, 1 - my_c), YAX | CORE)]

        def halves(parts):
            half = parts[0].shape[1] // 2
            return jnp.concatenate([p[:, :half] for p in parts]), jnp.concatenate([p[:, half:] for p in parts])

        def stack4(arr, far):
            return jnp.concatenate([arr, swap(arr, CORE), far, swap(far, CORE)], axis=0)

        x_full = lax.all_gather(x_loc, 'tp', axis=0, tiled=True)
        dy_all = lax.all_gather(dy_loc, 'tp', axis=0, tiled=True)
        seq_len, d_model = x_full.shape
        ff = w_up.shape[1]
        row_mean, row_rstd = norm_stats(x_full.astype(F32))
        h_mlp = norm_apply(x_full, row_mean, row_rstd, ln_params[2], ln_params[3])

        stats = jnp.concatenate([row_mean, row_rstd], axis=1)
        stats4 = jnp.concatenate([stats, swap(stats, CORE), swap(stats, XAX), swap(stats, XAX | CORE)], axis=0)
        x_parts = spread_x(x_full)
        ln_cols = shares_x(ln_params, my_x, my_c)

        h_mlp, _ = hold(h_mlp, x_parts[0])
        hidden, = hold(mm('td,df->tf', h_mlp, w_up).astype(BF16))
        h32 = hidden.astype(F32)
        cdf = 0.5 * (1.0 + lax.erf(h32 * (0.5 ** 0.5)))
        gelu_out, slope = hold((h32 * cdf).astype(BF16), cdf + h32 * (jnp.exp(-0.5 * h32 * h32) * 0.3989422804014327))
        gelu_parts = spread_y(gelu_out)

        x_again, gelu_parts[0] = hold(x_full, gelu_parts[0])
        h_attn = norm_apply(x_again, row_mean, row_rstd, ln_params[0], ln_params[1])
        qkv_proj = jnp.einsum('td,dgjh->tgjh', h_attn, w_qkv, preferred_element_type=F32).astype(BF16)[None]
        cos_t, sin_t = rope_tables(jnp.arange(seq_len), w_qkv.shape[3])
        context, attn_pull = jax.vjp(lambda qkv_in: attention_core(qkv_in, cos_t, sin_t), qkv_proj)
        ctx_parts = spread_y(context.reshape(seq_len, -1))
        mid = d_model // 2
        x_keep, x_send = halves(x_parts)
        norm4 = lambda rows, row, cols: norm_apply(rows, stats4[:, :1], stats4[:, 1:], ln_cols[row, cols], ln_cols[row + 1, cols])
        lo, hi = slice(0, x_keep.shape[1]), slice(x_keep.shape[1], None)
        ha_send, hm_send, ha_keep, hm_keep = hold(
            norm4(x_send, 0, hi), norm4(x_send, 2, hi), norm4(x_keep, 0, lo), norm4(x_keep, 2, lo))

        dy_full, tied = dy_all, dy_all
        dy_lo, dy_hi = hold(dy_full[:, :mid], dy_full[:, mid:])
        far_lo, far_hi = swap(dy_lo, YAX), swap(dy_hi, YAX)
        d_hidden, far_hidden = [], []
        for i in (0, 1):
            cols = slice(i * ff // 2, (i + 1) * ff // 2)
            d_gelu = mm('td,fd->tf', tied, w_down[cols]).astype(BF16)
            d_hid, = hold((d_gelu.astype(F32) * slope[:, cols]).astype(BF16))
            d_hidden.append(d_hid)
            far_hidden.append(swap(d_hid, XAX))
            tied, _ = hold(dy_full, d_hid)

        d_ctx = mm('td,cd->tc', tied, w_out).astype(BF16)
        (d_proj,) = attn_pull(d_ctx.reshape(context.shape))
        d_flat, = hold(d_proj.reshape(seq_len, -1))
        far_proj = swap(d_flat, XAX)
        d_hattn_part, = hold(mm('tk,dk->td', d_flat, w_qkv.reshape(d_model, -1)).astype(BF16))
        d_hattn = lax.psum_scatter(d_hattn_part, 'tp', scatter_dimension=0, tiled=True)
        gelu_keep, gelu_send = halves(gelu_parts)
        ctx_keep, ctx_send = halves(ctx_parts)

        grad = lambda lhs4, rhs4: hold(mm('tr,tc->rc', lhs4, rhs4))[0]
        after = lambda value, *earlier: hold(value, *earlier)[0]
        up4_0 = stack4(d_hidden[0], far_hidden[0])
        up0 = grad(after(hm_send, d_hattn_part), up4_0)
        came_up0 = swap(up0, YAX)
        dy4_0 = stack4(dy_lo, far_lo)
        hid_cat = jnp.concatenate(d_hidden, axis=1)
        d_hmlp_part, = hold(mm('tf,df->td', hid_cat, w_up).astype(BF16))
        d_hmlp = lax.psum_scatter(d_hmlp_part, 'tp', scatter_dimension=0, tiled=True)
        down0 = grad(gelu_send, dy4_0)
        came_down0 = swap(down0, XAX)
        up4_1 = stack4(d_hidden[1], after(far_hidden[1], down0))
        up1 = grad(after(hm_send, down0), up4_1)
        came_up1 = swap(up1, YAX)
        dy4_1 = stack4(dy_hi, after(far_hi, d_hmlp_part))
        down1 = grad(after(gelu_send, up1), dy4_1)
        came_down1 = swap(down1, XAX)
        qkv4 = stack4(d_flat, after(far_proj, down1))
        out0 = grad(after(ctx_send, down1), dy4_0)
        out1 = grad(after(ctx_send, out0), dy4_1)
        came_out = [swap(out0, XAX), swap(out1, XAX)]
        qkv0 = grad(after(ha_send, out1), qkv4)
        came_qkv = swap(qkv0, YAX)
        hm_keep, gelu_keep, ctx_keep, ha_keep, _ = hold(hm_keep, gelu_keep, ctx_keep, ha_keep, qkv0)
        kept_up = [grad(hm_keep, up4_0), grad(hm_keep, up4_1)]
        kept_down = [grad(gelu_keep, dy4_0), grad(gelu_keep, dy4_1)]
        kept_out = [grad(ctx_keep, dy4_0), grad(ctx_keep, dy4_1)]
        kept_qkv = grad(ha_keep, qkv4)
        d_hattn, d_hmlp = after(d_hattn, *kept_up, *kept_down), after(d_hmlp, *kept_up, *kept_down)

        x_loc_f32 = x_loc.astype(F32)
        _, attn_norm_pull = jax.vjp(layer_norm, x_loc_f32, ln_params[0], ln_params[1])
        _, mlp_norm_pull = jax.vjp(layer_norm, x_loc_f32, ln_params[2], ln_params[3])
        dx_attn, dgain_attn, dshift_attn = attn_norm_pull(d_hattn)
        dx_mlp, dgain_mlp, dshift_mlp = mlp_norm_pull(d_hmlp)
        grad_x = (dy_loc.astype(F32) + dx_attn + dx_mlp).astype(BF16)[None]
        grad_ln = jnp.stack([dgain_attn, dshift_attn, dgain_mlp, dshift_mlp])
        for bit in (1, 2):
            grad_ln = grad_ln + swap_tp(grad_ln, bit)
        grad_ln = grad_ln + swap(grad_ln, CORE)
        (kept_up[0], kept_up[1], kept_down[0], kept_down[1], kept_out[0], kept_out[1], kept_qkv, grad_x, grad_ln) = hold(
            *kept_up, *kept_down, *kept_out, kept_qkv, grad_x, grad_ln)
        for bit in (YAX, XAX):
            grad_ln = grad_ln + swap(grad_ln, bit)

        join = lambda kept, came: jnp.concatenate([k + c for k, c in zip(kept, came)], axis=1)
        grad_wqkv = (kept_qkv + came_qkv).reshape((-1,) + w_qkv.shape[1:])
        grad_wup = join(kept_up, (came_up0, came_up1))
        grad_wdown = join(kept_down, (came_down0, came_down1))
        return grad_x, grad_ln, grad_wqkv, join(kept_out, came_out), grad_wup, grad_wdown

    act_spec = P('dp', 'tp', None)
    in_specs = (act_spec, act_spec, P(None, None), P(None, 'tp', None, None), P('tp', None), P(None, 'tp'), P('tp', None))
    out_specs = (act_spec, P(None, None), P('dp', 'tp', None, None), P(('tp', 'dp'), None), P('dp', 'tp'), P(('tp', 'dp'), None))
    return jax.shard_map(local_body, mesh=mesh, in_specs=in_specs, out_specs=out_specs, check_vma=False)
```

```python
import jax
import jax.numpy as jnp
from jax import lax
from jax.sharding import PartitionSpec as P

NORM_EPS = 1e-5
ROPE_BASE = 10000.0
CORE, XAX, YAX = 1, 2, 4
F32, BF16 = jnp.float32, jnp.bfloat16


def norm_stats(x_rows):
    row_mean = jnp.mean(x_rows, axis=-1, keepdims=True)
    centered = x_rows - row_mean
    row_var = jnp.mean(centered * centered, axis=-1, keepdims=True)
    return row_mean, lax.rsqrt(row_var + NORM_EPS)


def norm_apply(x_rows, row_mean, row_rstd, norm_gain, norm_shift):
    return ((x_rows.astype(F32) - row_mean) * row_rstd * norm_gain + norm_shift).astype(BF16)


def layer_norm(x_rows, norm_gain, norm_shift):
    row_mean, row_rstd = norm_stats(x_rows)
    return norm_apply(x_rows, row_mean, row_rstd, norm_gain, norm_shift)


def rope_tables(positions, head_dim):
    half_dim = head_dim // 2
    inv_freq = ROPE_BASE ** (-2.0 * jnp.arange(half_dim, dtype=F32) / head_dim)
    angles = positions.astype(F32)[:, None] * inv_freq[None, :]
    return jnp.cos(angles), jnp.sin(angles)


def apply_rope(tensor, cos_t, sin_t):
    half_dim = tensor.shape[-1] // 2
    t_f32 = tensor.astype(F32)
    lo_half = t_f32[..., :half_dim]
    hi_half = t_f32[..., half_dim:]
    return jnp.concatenate([lo_half * cos_t - hi_half * sin_t, hi_half * cos_t + lo_half * sin_t], axis=-1).astype(BF16)


def attention_core(qkv_proj, cos_t, sin_t):
    q_slots = qkv_proj.shape[3] - 2
    positions = jnp.arange(qkv_proj.shape[1])
    rotated = apply_rope(qkv_proj[:, :, :, :q_slots + 1, :], cos_t[:, None, None, :], sin_t[:, None, None, :])
    query_rot = rotated[:, :, :, :q_slots, :]
    key_rot = rotated[:, :, :, q_slots, :]
    values = qkv_proj[:, :, :, q_slots + 1, :]
    scores = jnp.einsum('btgqh,bsgh->bgqts', query_rot, key_rot, preferred_element_type=F32) * (qkv_proj.shape[4] ** -0.5)
    causal = positions[:, None] >= positions[None, :]
    attn_probs = jax.nn.softmax(jnp.where(causal, scores, -1e30), axis=-1).astype(BF16)
    return jnp.einsum('bgqts,bsgh->btgqh', attn_probs, values, preferred_element_type=F32).astype(BF16)


def swap(value, bit):
    return lax.ppermute(value, 'dp', [(i, i ^ bit) for i in range(8)])


def swap_tp(value, bit):
    return lax.ppermute(value, 'tp', [(i, i ^ bit) for i in range(4)])


def hold(*values):
    return lax.optimization_barrier(values)


def mm(spec, lhs, rhs):
    return jnp.einsum(spec, lhs, rhs, preferred_element_type=F32)


def solution(mesh):
    def local_body(x_in, dy_in, ln_params, w_qkv, w_out, w_up, w_down):
        x_loc, dy_loc = x_in[0], dy_in[0]
        me = lax.axis_index('dp')
        my_c, my_x, my_y = me % 2, (me // 2) % 2, me // 4

        def shares_x(arr, x_at, c_at):
            width = arr.shape[1] // 8
            pick = lambda y: lax.dynamic_slice_in_dim(arr, (y * 4 + x_at * 2 + c_at) * width, width, 1)
            return jnp.concatenate([pick(my_y), pick(1 - my_y)], axis=1)

        def shares_y(arr, y_at, c_at):
            width = arr.shape[1] // 8
            pick = lambda x: lax.dynamic_slice_in_dim(arr, (y_at * 4 + x * 2 + c_at) * width, width, 1)
            return jnp.concatenate([pick(my_x), pick(1 - my_x)], axis=1)

        def spread_x(arr):
            return [shares_x(arr, my_x, my_c), swap(shares_x(arr, my_x, 1 - my_c), CORE),
                    swap(shares_x(arr, 1 - my_x, my_c), XAX),
                    swap(shares_x(arr, 1 - my_x, 1 - my_c), XAX | CORE)]

        def spread_y(arr):
            return [shares_y(arr, my_y, my_c), swap(shares_y(arr, my_y, 1 - my_c), CORE),
                    swap(shares_y(arr, 1 - my_y, my_c), YAX),
                    swap(shares_y(arr, 1 - my_y, 1 - my_c), YAX | CORE)]

        def halves(parts):
            half = parts[0].shape[1] // 2
            return jnp.concatenate([p[:, :half] for p in parts]), jnp.concatenate([p[:, half:] for p in parts])

        def stack4(arr, far):
            return jnp.concatenate([arr, swap(arr, CORE), far, swap(far, CORE)], axis=0)

        x_full = lax.all_gather(x_loc, 'tp', axis=0, tiled=True)
        dy_all = lax.all_gather(dy_loc, 'tp', axis=0, tiled=True)
        seq_len, d_model = x_full.shape
        ff = w_up.shape[1]
        row_mean, row_rstd = norm_stats(x_full.astype(F32))
        h_mlp = norm_apply(x_full, row_mean, row_rstd, ln_params[2], ln_params[3])

        stats = jnp.concatenate([row_mean, row_rstd], axis=1)
        stats4 = jnp.concatenate([stats, swap(stats, CORE), swap(stats, XAX), swap(stats, XAX | CORE)], axis=0)
        x_parts = spread_x(x_full)
        ln_cols = shares_x(ln_params, my_x, my_c)

        h_mlp, _ = hold(h_mlp, x_parts[0])
        hidden, = hold(mm('td,df->tf', h_mlp, w_up).astype(BF16))
        h32 = hidden.astype(F32)
        cdf = 0.5 * (1.0 + lax.erf(h32 * (0.5 ** 0.5)))
        gelu_out, slope = hold((h32 * cdf).astype(BF16), cdf + h32 * (jnp.exp(-0.5 * h32 * h32) * 0.3989422804014327))
        gelu_parts = spread_y(gelu_out)

        x_again, gelu_parts[0] = hold(x_full, gelu_parts[0])
        h_attn = norm_apply(x_again, row_mean, row_rstd, ln_params[0], ln_params[1])
        qkv_proj = jnp.einsum('td,dgjh->tgjh', h_attn, w_qkv, preferred_element_type=F32).astype(BF16)[None]
        cos_t, sin_t = rope_tables(jnp.arange(seq_len), w_qkv.shape[3])
        context, attn_pull = jax.vjp(lambda qkv_in: attention_core(qkv_in, cos_t, sin_t), qkv_proj)
        ctx_parts = spread_y(context.reshape(seq_len, -1))
        mid = d_model // 2
        x_keep, x_send = halves(x_parts)
        norm4 = lambda rows, row, cols: norm_apply(rows, stats4[:, :1], stats4[:, 1:], ln_cols[row, cols], ln_cols[row + 1, cols])
        lo, hi = slice(0, x_keep.shape[1]), slice(x_keep.shape[1], None)
        ha_send, hm_send, ha_keep, hm_keep = hold(
            norm4(x_send, 0, hi), norm4(x_send, 2, hi), norm4(x_keep, 0, lo), norm4(x_keep, 2, lo))

        dy_full, tied = dy_all, dy_all
        dy_lo, dy_hi = hold(dy_full[:, :mid], dy_full[:, mid:])
        far_lo, far_hi = swap(dy_lo, YAX), swap(dy_hi, YAX)
        d_hidden, far_hidden = [], []
        for i in (0, 1):
            cols = slice(i * ff // 2, (i + 1) * ff // 2)
            d_gelu = mm('td,fd->tf', tied, w_down[cols]).astype(BF16)
            d_hid, = hold((d_gelu.astype(F32) * slope[:, cols]).astype(BF16))
            d_hidden.append(d_hid)
            far_hidden.append(swap(d_hid, XAX))
            tied, _ = hold(dy_full, d_hid)

        tied, hm_send = hold(dy_full, hm_send)
        d_ctx = mm('td,cd->tc', tied, w_out).astype(BF16)
        (d_proj,) = attn_pull(d_ctx.reshape(context.shape))
        d_flat, = hold(d_proj.reshape(seq_len, -1))
        far_proj = swap(d_flat, XAX)
        d_hattn_part, = hold(mm('tk,dk->td', d_flat, w_qkv.reshape(d_model, -1)).astype(BF16))
        gelu_keep, gelu_send = halves(gelu_parts)
        gelu_send, d_hattn_part = hold(gelu_send, d_hattn_part)
        d_hattn = lax.psum_scatter(d_hattn_part, 'tp', scatter_dimension=0, tiled=True)
        ctx_keep, ctx_send = halves(ctx_parts)

        grad = lambda lhs4, rhs4: hold(mm('tr,tc->rc', lhs4, rhs4))[0]
        after = lambda value, *earlier: hold(value, *earlier)[0]
        up4_0 = stack4(d_hidden[0], far_hidden[0])
        up0 = grad(hm_send, up4_0)
        came_up0 = swap(up0, YAX)
        dy4_0 = stack4(dy_lo, far_lo)
        hid_cat = jnp.concatenate(d_hidden, axis=1)
        d_hmlp_part, = hold(mm('tf,df->td', hid_cat, w_up).astype(BF16))
        hm_send, d_hmlp_part = hold(hm_send, d_hmlp_part)
        d_hmlp = lax.psum_scatter(d_hmlp_part, 'tp', scatter_dimension=0, tiled=True)
        down0 = grad(gelu_send, dy4_0)
        came_down0 = swap(down0, XAX)
        up4_1 = stack4(d_hidden[1], after(far_hidden[1], down0))
        up1 = grad(after(hm_send, down0), up4_1)
        came_up1 = swap(up1, YAX)
        dy4_1 = stack4(dy_hi, after(far_hi, d_hmlp_part))
        down1 = grad(after(gelu_send, up1), dy4_1)
        came_down1 = swap(down1, XAX)
        qkv4 = stack4(d_flat, after(far_proj, down1))
        out0 = grad(after(ctx_send, down1), dy4_0)
        out1 = grad(after(ctx_send, out0), dy4_1)
        came_out = [swap(out0, XAX), swap(out1, XAX)]
        qkv0 = grad(after(ha_send, out1), qkv4)
        came_qkv = swap(qkv0, YAX)
        hm_keep, gelu_keep, ctx_keep, ha_keep, _ = hold(hm_keep, gelu_keep, ctx_keep, ha_keep, qkv0)
        kept_up = [grad(hm_keep, up4_0), grad(hm_keep, up4_1)]
        kept_down = [grad(gelu_keep, dy4_0), grad(gelu_keep, dy4_1)]
        kept_out = [grad(ctx_keep, dy4_0), grad(ctx_keep, dy4_1)]
        kept_qkv = grad(ha_keep, qkv4)
        d_hattn, d_hmlp = after(d_hattn, *kept_up, *kept_down), after(d_hmlp, *kept_up, *kept_down)

        x_loc_f32 = x_loc.astype(F32)
        _, attn_norm_pull = jax.vjp(layer_norm, x_loc_f32, ln_params[0], ln_params[1])
        _, mlp_norm_pull = jax.vjp(layer_norm, x_loc_f32, ln_params[2], ln_params[3])
        dx_attn, dgain_attn, dshift_attn = attn_norm_pull(d_hattn)
        dx_mlp, dgain_mlp, dshift_mlp = mlp_norm_pull(d_hmlp)
        grad_x = (dy_loc.astype(F32) + dx_attn + dx_mlp).astype(BF16)[None]
        grad_ln = jnp.stack([dgain_attn, dshift_attn, dgain_mlp, dshift_mlp])
        for bit in (1, 2):
            grad_ln = grad_ln + swap_tp(grad_ln, bit)
        grad_ln = grad_ln + swap(grad_ln, CORE)
        (kept_up[0], kept_up[1], kept_down[0], kept_down[1], kept_out[0], kept_out[1], kept_qkv, grad_x, grad_ln) = hold(
            *kept_up, *kept_down, *kept_out, kept_qkv, grad_x, grad_ln)
        grad_ln = (grad_ln + swap(grad_ln, XAX)) + (swap(grad_ln, YAX) + swap(grad_ln, YAX | XAX))

        join = lambda kept, came: jnp.concatenate([k + c for k, c in zip(kept, came)], axis=1)
        grad_wqkv = (kept_qkv + came_qkv).reshape((-1,) + w_qkv.shape[1:])
        grad_wup = join(kept_up, (came_up0, came_up1))
        grad_wdown = join(kept_down, (came_down0, came_down1))
        kept_out[0], kept_out[1], grad_wqkv, grad_wup, grad_wdown = hold(*kept_out, grad_wqkv, grad_wup, grad_wdown)
        return grad_x, grad_ln, grad_wqkv, join(kept_out, came_out), grad_wup, grad_wdown

    act_spec = P('dp', 'tp', None)
    in_specs = (act_spec, act_spec, P(None, None), P(None, 'tp', None, None), P('tp', None), P(None, 'tp'), P('tp', None))
    out_specs = (act_spec, P(None, None), P('dp', 'tp', None, None), P(('tp', 'dp'), None), P('dp', 'tp'), P(('tp', 'dp'), None))
    return jax.shard_map(local_body, mesh=mesh, in_specs=in_specs, out_specs=out_specs, check_vma=False)
```
